128 devices in a mesh: grp: 16 (over z_hi, y, core), loc: 8 (over z_lo, x).
Axes of the slice: x: 4, y: 4, z: 4 (z_hi: 2, z_lo: 2; z = z_hi * 2 + z_lo), core: 2. Of those that a mesh axis runs over, the one named last changes fastest.
Arguments:
- tokens: bfloat16 [16384, 7168], P(('grp', 'loc')), may hold values from -6 to 6
- route: int32 [16384, 1], P(('grp', 'loc')), may hold values from 0 to 31; in each aligned block of 128 rows (0 to 127, 128 to 255, ...) at most 5 rows name the same one
- gate_prob: float32 [16384, 1], P(('grp', 'loc')), may hold values from 0.25 to 1
- w_gate: bfloat16 [128, 7168, 256], P(('grp', 'loc')), may hold values from -0.0625 to 0.0625
- w_up: bfloat16 [128, 7168, 256], P(('grp', 'loc')), may hold values from -0.0625 to 0.0625
- w_down: bfloat16 [128, 256, 7168], P(('grp', 'loc')), may hold values from -0.1875 to 0.1875
- partner: int32 [128, 2], replicated, may hold values from 0 to 127, as said below
Outputs:
- mixed: bfloat16 [16384, 7168], P(('grp', 'loc'))
The draws below stay inside these ranges and needn't reach their ends.
Inputs may be any that keep to these rules, and one draw needn't show every extreme that they name: `route`: within the 128 rows of one device no expert is named more than 5 times, a bound that some block reaches. partner[i, h] is slot i itself, slot i - 1 or slot i + 1, cyclically over all slots.
All inputs are finite; a program needn't handle non-finite values.
Results may differ from the reference program's by a relative error of at most 0.0056.
Values may be sent and summed in bfloat16 or wider, within the bound.
No kernel may reach another device: no remote copies, remote signals or barrier semaphores. Data moves between devices by JAX's collectives and lax.ppermute only.
A program may use at most 192 MiB of HBM per device.

```python
import math
import jax
import jax.numpy as jnp
import numpy as np
from jax import lax

D = 7168
FFW = 1024
SPAN = 4
TOP = 1
TOK_DEV = 128
HID = 256
EXPERTS = 32
TOKENS = 16384
CAP = 5
N_GRP = 16
N_LOC = 8


def draw_partner(key, part):
    slots_all = EXPERTS * SPAN
    index_all = jnp.arange(slots_all, dtype=jnp.int32)
    offsets = jax.random.randint(jax.random.fold_in(key, 11), (slots_all, 2), -1, 2).astype(jnp.int32)
    middle = slots_all // 2
    offsets = offsets.at[0, 0].set(-1).at[0, 1].set(1)
    offsets = offsets.at[middle, 0].set(-1).at[middle, 1].set(1)
    offsets = offsets.at[middle - 1, 0].set(1).at[middle - 1, 1].set(-1)
    offsets = offsets.at[slots_all - 1, 0].set(1).at[slots_all - 1, 1].set(-1)
    return ((index_all[:, None] + offsets) % slots_all).astype(jnp.int32)


def level_of(own_key, shape, pieces, least, largest):
    level = 1.0
    for dim, parts in pieces:
        steps = jax.random.uniform(jax.random.fold_in(jax.random.fold_in(own_key, 6), dim), (parts,), jnp.float32, least / len(pieces), largest / len(pieces))
        level = level * jnp.repeat(jnp.exp(steps), shape[dim] // parts).reshape((-1,) + (1,) * (len(shape) - 1 - dim))
    return level


def deal_out(own_key, own, number, rows, number_of, top, limit, skew):
    order = jax.random.permutation(own_key, number_of)
    packed, usual = portions_of(number_of, rows * top, limit, skew, True), portions_of(number_of, rows * top, limit, skew, False)
    places = jnp.arange(number_of)

    def named(tallies, turn):
        used = int((tallies > 0).sum())
        fixed = max(1, used // 4)
        passed = fixed + (places - fixed + turn * (used - fixed)) % max(1, number_of - fixed)
        return jnp.zeros((number_of,), jnp.int32).at[order[jnp.where(places < fixed, places, passed)]].set(jnp.asarray(tallies, jnp.int32))

    tallies = jnp.where(number % 4 == 0, named(packed, number // 4), named(usual, number - number // 4 - 1))
    mixed = jax.random.permutation(jax.random.fold_in(own, 3), number_of)
    source_of, sink = mixed[0:number_of // 2 * 2:2], mixed[1:number_of // 2 * 2:2]
    slack = jnp.minimum(tallies[source_of] - 1, limit - tallies[sink]) // 2
    slack = jnp.where((source_of == order[0]) | (sink == order[0]) | (tallies[sink] == 0), 0, jnp.maximum(slack, 0))
    passed = jax.random.randint(jax.random.fold_in(own, 4), (number_of // 2,), 0, 1 << 20) % (slack + 1)
    tallies = tallies.at[source_of].add(-passed).at[sink].add(passed)
    members = jnp.searchsorted(jnp.cumsum(tallies), jnp.arange(rows * top), side="right").astype(jnp.int32)
    grid = members.reshape(top, rows).T
    grid = grid[jax.random.permutation(jax.random.fold_in(own, 1), rows)]
    turn = jax.random.randint(jax.random.fold_in(own, 2), (rows, 1), 0, top)
    return jnp.take_along_axis(grid, (jnp.arange(top)[None, :] + turn) % top, axis=1)


def portions_of(amount, total, bound, skew, full):
    weights = [(1 << 20) // math.isqrt(grade ** skew) + 1 for grade in range(1, amount + 1)]
    largest = bound if full else min(bound, max(-(-total // amount), total * weights[0] // sum(weights)))
    least = 1 if total - largest >= amount - 1 else 0
    holding, spare = [largest] + [least] * (amount - 1), total - largest - least * (amount - 1)
    while spare > 0:
        candidates = [i for i in range(1, amount) if holding[i] < largest] or [i for i in range(1, amount) if holding[i] < bound]
        whole, remaining = sum([weights[i] for i in candidates]), spare
        for i in candidates:
            extra = min(bound - holding[i], max(1, remaining * weights[i] // whole), spare)
            holding[i] = holding[i] + extra
            spare = spare - extra
    return np.array(holding)


def bell_draw(rng, extent, spread, reach, cuts=(), kind=jnp.bfloat16):
    loudness = level_of(rng, extent, cuts, -0.22, 0.18) if cuts else 1.0
    array = jax.random.normal(rng, extent, jnp.float32) * spread * loudness
    return jnp.minimum(jnp.maximum(array, -reach), reach).astype(kind)


def setup_inputs(seed: int = 0) -> dict:
    seeds = jax.random.split(jax.random.key(seed), 8)
    tokens = bell_draw(seeds[0], (TOKENS, D), 1.0, 6.0, ((0, 128),))
    route_keys = jax.random.split(jax.random.fold_in(seeds[1], 1), TOKENS // TOK_DEV)
    route_turns = jax.random.permutation(jax.random.fold_in(seeds[1], 3), TOKENS // TOK_DEV)
    route = jax.vmap(lambda own, number: deal_out(jax.random.fold_in(seeds[1], 2), own, number, TOK_DEV, EXPERTS, TOP, CAP, 1))(route_keys, route_turns).reshape((TOKENS, TOP))
    gate_prob = jnp.clip(jnp.exp(math.log(1.0) - 1.3862944 * jax.random.uniform(seeds[2], (TOKENS, TOP), jnp.float32) ** level_of(seeds[2], (TOKENS, TOP), ((0, 128),), -0.2, 0.2)), 0.25, 1.0)
    w_gate = bell_draw(seeds[3], (N_GRP * N_LOC, D, HID), D ** -0.5, 0.0625, ((0, 128),))
    w_up = bell_draw(seeds[4], (N_GRP * N_LOC, D, HID), D ** -0.5, 0.0625, ((0, 128),))
    w_down = bell_draw(seeds[5], (N_GRP * N_LOC, HID, D), FFW ** -0.5, 0.1875, ((0, 128),))
    partner = draw_partner(jax.random.fold_in(seeds[7], 71), 0)
    return {"tokens": tokens, "route": route, "gate_prob": gate_prob, "w_gate": w_gate, "w_up": w_up, "w_down": w_down, "partner": partner}


def expert_pass(row_block, gate_block, up_block, down_block):
    gate_part = jnp.dot(row_block, gate_block, preferred_element_type=jnp.float32)
    up_part = jnp.dot(row_block, up_block, preferred_element_type=jnp.float32)
    hidden = (jax.nn.silu(gate_part) * up_part).astype(jnp.bfloat16)
    return jnp.dot(hidden, down_block, preferred_element_type=jnp.float32).astype(jnp.bfloat16)


def reference(tokens, route, gate_prob, w_gate, w_up, w_down, partner):
    slots_all = N_GRP * N_LOC
    per_source = TOK_DEV * TOP
    half = HID // 2
    routes = route.reshape(slots_all, per_source).astype(jnp.int32)
    onehot = (routes[:, :, None] == jnp.arange(EXPERTS, dtype=jnp.int32)[None, None, :]).astype(jnp.int32)
    slot_rank = (jnp.sum(jnp.cumsum(onehot, axis=1) * onehot, axis=2) - 1).astype(jnp.int32)
    assign_index = jnp.arange(slots_all * per_source, dtype=jnp.int32).reshape(slots_all, per_source)
    sources = jnp.broadcast_to(jnp.arange(slots_all, dtype=jnp.int32)[:, None], (slots_all, per_source))
    table = jnp.full((EXPERTS, slots_all, CAP), slots_all * per_source, jnp.int32)
    table = table.at[routes, sources, slot_rank].set(assign_index)
    padded = jnp.concatenate([jnp.repeat(tokens, TOP, axis=0), jnp.zeros((1, D), tokens.dtype)], axis=0)

    def expert_step(carry, expert_id):
        picks = table[expert_id].reshape(-1)
        row_block = padded[picks]
        total = jnp.zeros((slots_all * CAP, D), jnp.float32)
        for block_id in range(SPAN):
            first = partner[expert_id * SPAN + block_id, 0]
            second = partner[expert_id * SPAN + block_id, 1]
            gate_block = jnp.concatenate([w_gate[first][:, :half], w_gate[second][:, half:]], axis=1)
            up_block = jnp.concatenate([w_up[first][:, :half], w_up[second][:, half:]], axis=1)
            down_block = jnp.concatenate([w_down[first][:half], w_down[second][half:]], axis=0)
            total = total + expert_pass(row_block, gate_block, up_block, down_block).astype(jnp.float32)
        carry = carry.at[picks].set(total, mode="drop")
        return carry, expert_id

    mixed_rows = lax.scan(expert_step, jnp.zeros((slots_all * per_source, D), jnp.float32),
                          jnp.arange(EXPERTS, dtype=jnp.int32))[0]
    weighted = mixed_rows * gate_prob.reshape(-1)[:, None]
    return jnp.sum(weighted.reshape(TOKENS, TOP, D), axis=1).astype(jnp.bfloat16)
```

```python
import jax
import jax.numpy as jnp
from jax import lax
from jax.sharding import Mesh, PartitionSpec as P

SPAN = 4
CAPACITY = 5
PLANE = ("zh", "y", "c", "zl")
EVERY = PLANE + ("x",)
LANES = 128


def neighbours(step):
    return [(i, (i + step) % SPAN) for i in range(SPAN)]


def shift(block, step):
    return lax.ppermute(block, "x", neighbours(step))


def edge_pairs(which, experts):
    pairs = []
    for e in range(experts):
        pairs.append((SPAN * e + SPAN - 1, SPAN * ((e + 1) % experts) + which))
        pairs.append((SPAN * e, SPAN * ((e - 1) % experts) + SPAN - 1 - which))
    return pairs


def edge_blocks(w_gate, w_up, w_down, experts):
    quarter = w_gate.shape[1] // SPAN
    into, out = [], []
    for which in range(SPAN):
        cut = slice(which * quarter, (which + 1) * quarter)
        pairs = edge_pairs(which, experts)
        into.append(lax.ppermute(jnp.concatenate([w_gate[:, cut], w_up[:, cut]], axis=1), EVERY, pairs))
        out.append(lax.ppermute(w_down[cut], EVERY, pairs))
    return into, out


def multiplicities(partner, own, slots):
    expert, place = own // SPAN, own % SPAN
    first = expert * SPAN
    mine = lax.dynamic_slice_in_dim(partner, first, SPAN, 0)
    kept = jnp.sum((mine == own).astype(jnp.float32), axis=0)
    low = (mine[0] == (first - 1) % slots).astype(jnp.float32)
    high = (mine[SPAN - 1] == (first + SPAN) % slots).astype(jnp.float32)
    early = jnp.where(place < 2, low[0], high[0])
    late = jnp.where(place < 2, high[1], low[1])
    return kept, early, late


def dot(a, b):
    return jnp.dot(a, b, preferred_element_type=jnp.float32)


def body(tokens, route, gate_prob, w_gate, w_up, w_down, partner):
    slots = lax.axis_size(EVERY)
    own = lax.axis_index(EVERY)
    experts = slots // SPAN
    place = own % SPAN
    width = tokens.shape[1]
    w_gate, w_up, w_down = w_gate[0], w_up[0], w_down[0]
    quarter = w_gate.shape[1] // SPAN
    into, out = edge_blocks(w_gate, w_up, w_down, experts)

    flat_route = route.reshape(-1)
    onehot = (flat_route[:, None] == jnp.arange(experts, dtype=jnp.int32)[None, :]).astype(jnp.int32)
    rank = jnp.sum(jnp.cumsum(onehot, axis=0) * onehot, axis=1) - 1
    row = flat_route * CAPACITY + rank
    rows = experts * CAPACITY
    picker = (jnp.arange(rows, dtype=jnp.int32)[:, None] == row[None, :]).astype(jnp.bfloat16)
    outgoing = dot(picker, tokens).astype(jnp.bfloat16)
    tiled = (experts, CAPACITY, width // LANES, LANES)
    arrived = lax.all_to_all(outgoing.reshape(tiled), PLANE, 0, 0, tiled=True)
    mid = arrived.reshape(rows, width)
    half = rows // 2

    a, b = mid[:half], mid[half:]
    from_left_a = shift(a, 1)
    from_right_b = shift(b, -1)
    from_left_b = shift(b, 1)
    from_right_a = shift(a, -1)
    far_a = shift(from_left_a, 1)
    far_b = shift(from_right_b, -1)

    kept, early, late = multiplicities(partner, own, slots)
    scale = jnp.repeat(kept, 2 * quarter)[None, :]
    outer = (place == 0) | (place == SPAN - 1)
    piece_into = jnp.concatenate(
        [jnp.where(outer, into[0], into[1]), jnp.where(outer, into[3], into[2])], axis=1
    )
    piece_out = jnp.concatenate(
        [jnp.where(outer, out[0], out[1]), jnp.where(outer, out[3], out[2])], axis=0
    )
    down = jnp.concatenate([w_down, piece_out], axis=0)

    def partial(block):
        kept_hidden = jax.nn.silu(dot(block, w_gate)) * dot(block, w_up) * scale
        both = dot(block, piece_into)
        q = quarter
        hidden_early = jax.nn.silu(both[:, :q]) * both[:, q : 2 * q] * early
        hidden_late = jax.nn.silu(both[:, 2 * q : 3 * q]) * both[:, 3 * q :] * late
        hidden = jnp.concatenate([kept_hidden, hidden_early, hidden_late], axis=1).astype(jnp.bfloat16)
        return dot(hidden, down).astype(jnp.bfloat16)

    far = partial(jnp.concatenate([far_a, far_b], axis=0))
    right = partial(jnp.concatenate([from_right_a, from_right_b], axis=0))
    left = partial(jnp.concatenate([from_left_a, from_left_b], axis=0))
    home = partial(mid)

    def added(u, v):
        return (u.astype(jnp.float32) + v.astype(jnp.float32)).astype(jnp.bfloat16)

    to_right_a = shift(added(right[:half], shift(far[:half], 1)), 1)
    to_right_b = shift(right[half:], 1)
    to_left_b = shift(added(left[half:], shift(far[half:], -1)), -1)
    to_left_a = shift(left[:half], -1)
    f32 = jnp.float32
    total_a = home[:half].astype(f32) + to_right_a.astype(f32) + to_left_a.astype(f32)
    total_b = home[half:].astype(f32) + to_right_b.astype(f32) + to_left_b.astype(f32)
    total = jnp.concatenate([total_a, total_b], axis=0).astype(jnp.bfloat16)
    returned = lax.all_to_all(total.reshape(tiled), PLANE, 0, 0, tiled=True).reshape(rows, width)
    expert_out = lax.dot_general(picker, returned, (((0,), (0,)), ((), ())), preferred_element_type=f32)
    return (expert_out * gate_prob.reshape(-1)[:, None]).astype(jnp.bfloat16)


def solution(mesh):
    grid = Mesh(mesh.devices.reshape(2, 4, 2, 2, 4), EVERY)
    spec2, spec3 = P(EVERY, None), P(EVERY, None, None)
    return jax.shard_map(
        body,
        mesh=grid,
        in_specs=(spec2, spec2, spec2, spec3, spec3, spec3, P()),
        out_specs=spec2,
        check_vma=False,
    )
```

```python
import jax
import jax.numpy as jnp
from jax import lax
from jax.experimental import pallas as pl
from jax.experimental.pallas import tpu as pltpu
from jax.sharding import Mesh, PartitionSpec as P


SPAN = 4
CAPACITY = 5
PLANE = ("zh", "y", "c", "zl")
EVERY = PLANE + ("x",)
LANES = 128
CHUNK = 1024


def neighbours(step):
    return [(i, (i + step) % SPAN) for i in range(SPAN)]


def shift(block, step):
    return lax.ppermute(block, "x", neighbours(step))


def edge_pairs(which, experts):
    pairs = []
    for e in range(experts):
        pairs.append((SPAN * e + SPAN - 1, SPAN * ((e + 1) % experts) + which))
        pairs.append((SPAN * e, SPAN * ((e - 1) % experts) + SPAN - 1 - which))
    return pairs


def split_kernel(gate, up, down, *pieces):
    quarter = gate.shape[1] // SPAN
    for q, piece in enumerate(pieces):
        cut = slice(q * quarter, (q + 1) * quarter)
        piece[:CHUNK, :] = jnp.concatenate([gate[:, cut], up[:, cut]], axis=1)
        for t in range(CHUNK // LANES):
            piece[pl.ds(CHUNK + t * quarter, quarter), :] = down[cut, t * LANES : (t + 1) * LANES]


def split_pieces(w_gate, w_up, w_down):
    width, hidden = w_gate.shape
    chunks = width // CHUNK
    rows = CHUNK + CHUNK // LANES * (hidden // SPAN)
    return pl.pallas_call(
        split_kernel,
        grid=(chunks,),
        in_specs=[
            pl.BlockSpec((CHUNK, hidden), lambda i: (i, 0)),
            pl.BlockSpec((CHUNK, hidden), lambda i: (i, 0)),
            pl.BlockSpec((hidden, CHUNK), lambda i: (0, i)),
        ],
        out_specs=[pl.BlockSpec((rows, LANES), lambda i: (i, 0))] * SPAN,
        out_shape=[jax.ShapeDtypeStruct((chunks * rows, LANES), jnp.bfloat16)] * SPAN,
        name="split_pieces",
    )(w_gate, w_up, w_down)


def join_kernel(outer, p0, p1, p2, p3, into, down):
    quarter = LANES // 2

    def fill(first, second):
        gate = [first[:CHUNK, :quarter], second[:CHUNK, :quarter]]
        up = [first[:CHUNK, quarter:], second[:CHUNK, quarter:]]
        into[...] = jnp.concatenate(gate + up, axis=1)
        for t in range(CHUNK // LANES):
            lanes = slice(t * LANES, (t + 1) * LANES)
            down[:quarter, lanes] = first[pl.ds(CHUNK + t * quarter, quarter), :]
            down[quarter:, lanes] = second[pl.ds(CHUNK + t * quarter, quarter), :]

    @pl.when(outer[0] == 1)
    def _():
        fill(p0, p3)

    @pl.when(outer[0] == 0)
    def _():
        fill(p1, p2)


def join_pieces(outer, pieces, width):
    chunks = width // CHUNK
    rows = pieces[0].shape[0] // chunks
    on = pl.BlockSpec((rows, LANES), lambda i, s: (i * s[0], 0))
    off = pl.BlockSpec((rows, LANES), lambda i, s: (i * (1 - s[0]), 0))
    return pl.pallas_call(
        join_kernel,
        grid_spec=pltpu.PrefetchScalarGridSpec(
            num_scalar_prefetch=1,
            grid=(chunks,),
            in_specs=[on, off, off, on],
            out_specs=[
                pl.BlockSpec((CHUNK, 2 * LANES), lambda i, s: (i, 0)),
                pl.BlockSpec((LANES, CHUNK), lambda i, s: (0, i)),
            ],
        ),
        out_shape=[
            jax.ShapeDtypeStruct((width, 2 * LANES), jnp.bfloat16),
            jax.ShapeDtypeStruct((LANES, width), jnp.bfloat16),
        ],
        name="join_pieces",
    )(outer, *pieces)


def multiplicities(partner, own, slots):
    expert, place = own // SPAN, own % SPAN
    first = expert * SPAN
    mine = lax.dynamic_slice_in_dim(partner, first, SPAN, 0)
    kept = jnp.sum((mine == own).astype(jnp.float32), axis=0)
    low = (mine[0] == (first - 1) % slots).astype(jnp.float32)
    high = (mine[SPAN - 1] == (first + SPAN) % slots).astype(jnp.float32)
    early = jnp.where(place < 2, low[0], high[0])
    late = jnp.where(place < 2, high[1], low[1])
    return kept, jnp.stack([early, late])


def dot(a, b):
    return jnp.dot(a, b, preferred_element_type=jnp.float32)


def body(tokens, route, gate_prob, w_gate, w_up, w_down, partner):
    slots = lax.axis_size(EVERY)
    own = lax.axis_index(EVERY)
    experts = slots // SPAN
    place = lax.axis_index("x")
    width = tokens.shape[1]
    w_gate, w_up, w_down = w_gate[0], w_up[0], w_down[0]
    hidden = w_gate.shape[1]

    flat_route = route.reshape(-1)
    onehot = (flat_route[:, None] == jnp.arange(experts, dtype=jnp.int32)[None, :]).astype(jnp.int32)
    rank = jnp.sum(jnp.cumsum(onehot, axis=0) * onehot, axis=1) - 1
    row = flat_route * CAPACITY + rank
    rows = experts * CAPACITY
    picker = (jnp.arange(rows, dtype=jnp.int32)[:, None] == row[None, :]).astype(jnp.bfloat16)
    outgoing = dot(picker, tokens).astype(jnp.bfloat16)
    tiled = (experts, CAPACITY, width // LANES, LANES)
    outgoing, *held = lax.optimization_barrier((outgoing.reshape(tiled), w_gate, w_up, w_down))
    arrived = lax.all_to_all(outgoing, PLANE, 0, 0, tiled=True)
    pieces = [lax.ppermute(p, EVERY, edge_pairs(q, experts)) for q, p in enumerate(split_pieces(*held))]
    mid = arrived.reshape(rows, width)
    half = rows // 2

    a, b = mid[:half], mid[half:]
    from_left_a = shift(a, 1)
    from_right_b = shift(b, -1)
    from_left_b = shift(b, 1)
    from_right_a = shift(a, -1)
    far_a = shift(from_left_a, 1)
    far_b = shift(from_right_b, -1)

    kept, edge = multiplicities(partner, own, slots)
    scale = jnp.repeat(kept, hidden // 2)[None, :]
    edge_scale = jnp.repeat(edge, LANES // 2)[None, :]
    outer = ((place == 0) | (place == SPAN - 1)).astype(jnp.int32).reshape(1)
    *pieces, far_a, far_b = lax.optimization_barrier((*pieces, far_a, far_b))
    edge_into, edge_down = join_pieces(outer, pieces, width)
    down = jnp.concatenate([w_down, edge_down], axis=0)

    def partial(block):
        kept_hidden = jax.nn.silu(dot(block, w_gate)) * dot(block, w_up) * scale
        both = dot(block, edge_into)
        edge_hidden = jax.nn.silu(both[:, :LANES]) * both[:, LANES:] * edge_scale
        return dot(
            jnp.concatenate([kept_hidden, edge_hidden], axis=1).astype(jnp.bfloat16), down
        ).astype(jnp.bfloat16)

    far = partial(jnp.concatenate([far_a, far_b], axis=0))
    right = partial(jnp.concatenate([from_right_a, from_right_b], axis=0))
    left = partial(jnp.concatenate([from_left_a, from_left_b], axis=0))
    home = partial(mid)

    def added(u, v):
        return (u.astype(jnp.float32) + v.astype(jnp.float32)).astype(jnp.bfloat16)

    to_right_a = shift(added(right[:half], shift(far[:half], 1)), 1)
    to_right_b = shift(right[half:], 1)
    to_left_b = shift(added(left[half:], shift(far[half:], -1)), -1)
    to_left_a = shift(left[:half], -1)
    f32 = jnp.float32
    total_a = home[:half].astype(f32) + to_right_a.astype(f32) + to_left_a.astype(f32)
    total_b = home[half:].astype(f32) + to_right_b.astype(f32) + to_left_b.astype(f32)
    total = jnp.concatenate([total_a, total_b], axis=0).astype(jnp.bfloat16)
    returned = lax.all_to_all(total.reshape(tiled), PLANE, 0, 0, tiled=True).reshape(rows, width)
    expert_out = lax.dot_general(picker, returned, (((0,), (0,)), ((), ())), preferred_element_type=f32)
    return (expert_out * gate_prob.reshape(-1)[:, None]).astype(jnp.bfloat16)


def solution(mesh):
    grid = Mesh(mesh.devices.reshape(2, 4, 2, 2, 4), EVERY)
    spec2, spec3 = P(EVERY, None), P(EVERY, None, None)
    return jax.shard_map(
        body,
        mesh=grid,
        in_specs=(spec2, spec2, spec2, spec3, spec3, spec3, P()),
        out_specs=spec2,
        check_vma=False,
    )
```

```python
import jax
import jax.numpy as jnp
from jax import lax
from jax.experimental import pallas as pl
from jax.experimental.pallas import tpu as pltpu
from jax.sharding import Mesh, PartitionSpec as P


SPAN = 4
CAPACITY = 5
PLANE = ("zh", "y", "c", "zl")
EVERY = PLANE + ("x",)
LANES = 128
CHUNK = 1024


def neighbours(step):
    return [(i, (i + step) % SPAN) for i in range(SPAN)]


def shift(block, step):
    return lax.ppermute(block, "x", neighbours(step))


def cross_pairs(which):
    return [(SPAN - 1, which), (0, SPAN - 1 - which)]


def pass_pairs(which, experts):
    pairs = []
    for e in range(experts):
        pairs.append((SPAN * e + which, SPAN * ((e + 1) % experts) + which))
        pairs.append((SPAN * e + SPAN - 1 - which, SPAN * ((e - 1) % experts) + SPAN - 1 - which))
    return pairs


def split_kernel(gate, up, down, *pieces):
    quarter = gate.shape[1] // SPAN
    for q, piece in enumerate(pieces):
        cut = slice(q * quarter, (q + 1) * quarter)
        piece[:CHUNK, :] = jnp.concatenate([gate[:, cut], up[:, cut]], axis=1)
        for t in range(CHUNK // LANES):
            piece[pl.ds(CHUNK + t * quarter, quarter), :] = down[cut, t * LANES : (t + 1) * LANES]


def split_pieces(w_gate, w_up, w_down):
    width, hidden = w_gate.shape
    chunks = width // CHUNK
    rows = CHUNK + CHUNK // LANES * (hidden // SPAN)
    return pl.pallas_call(
        split_kernel,
        grid=(chunks,),
        in_specs=[
            pl.BlockSpec((CHUNK, hidden), lambda i: (i, 0)),
            pl.BlockSpec((CHUNK, hidden), lambda i: (i, 0)),
            pl.BlockSpec((hidden, CHUNK), lambda i: (0, i)),
        ],
        out_specs=[pl.BlockSpec((rows, LANES), lambda i: (i, 0))] * SPAN,
        out_shape=[jax.ShapeDtypeStruct((chunks * rows, LANES), jnp.bfloat16)] * SPAN,
        name="split_pieces",
    )(w_gate, w_up, w_down)


def join_kernel(outer, p0, p1, p2, p3, into, down):
    quarter = LANES // 2

    def fill(first, second):
        into[:, :LANES] = first[:CHUNK, :]
        into[:, LANES:] = second[:CHUNK, :]
        for t in range(CHUNK // LANES):
            lanes = slice(t * LANES, (t + 1) * LANES)
            down[:quarter, lanes] = first[pl.ds(CHUNK + t * quarter, quarter), :]
            down[quarter:, lanes] = second[pl.ds(CHUNK + t * quarter, quarter), :]

    @pl.when(outer[0] == 1)
    def _():
        fill(p0, p3)

    @pl.when(outer[0] == 0)
    def _():
        fill(p1, p2)


def join_pieces(outer, pieces, width):
    chunks = width // CHUNK
    rows = pieces[0].shape[0] // chunks
    on = pl.BlockSpec((rows, LANES), lambda i, s: (i * s[0], 0))
    off = pl.BlockSpec((rows, LANES), lambda i, s: (i * (1 - s[0]), 0))
    return pl.pallas_call(
        join_kernel,
        grid_spec=pltpu.PrefetchScalarGridSpec(
            num_scalar_prefetch=1,
            grid=(chunks,),
            in_specs=[on, off, off, on],
            out_specs=[
                pl.BlockSpec((CHUNK, 2 * LANES), lambda i, s: (i, 0)),
                pl.BlockSpec((LANES, CHUNK), lambda i, s: (0, i)),
            ],
        ),
        out_shape=[
            jax.ShapeDtypeStruct((width, 2 * LANES), jnp.bfloat16),
            jax.ShapeDtypeStruct((LANES, width), jnp.bfloat16),
        ],
        name="join_pieces",
    )(outer, *pieces)


def multiplicities(partner, own, slots):
    expert, place = own // SPAN, own % SPAN
    first = expert * SPAN
    mine = lax.dynamic_slice_in_dim(partner, first, SPAN, 0)
    kept = jnp.sum((mine == own).astype(jnp.float32), axis=0)
    low = (mine[0] == (first - 1) % slots).astype(jnp.float32)
    high = (mine[SPAN - 1] == (first + SPAN) % slots).astype(jnp.float32)
    early = jnp.where(place < 2, low[0], high[0])
    late = jnp.where(place < 2, high[1], low[1])
    return kept, jnp.stack([early, late])


def dot(a, b):
    return jnp.dot(a, b, preferred_element_type=jnp.float32)


def body(tokens, route, gate_prob, w_gate, w_up, w_down, partner):
    slots = lax.axis_size(EVERY)
    own = lax.axis_index(EVERY)
    experts = slots // SPAN
    place = lax.axis_index("x")
    width = tokens.shape[1]
    w_gate, w_up, w_down = w_gate[0], w_up[0], w_down[0]
    hidden = w_gate.shape[1]

    flat_route = route.reshape(-1)
    onehot = (flat_route[:, None] == jnp.arange(experts, dtype=jnp.int32)[None, :]).astype(jnp.int32)
    rank = jnp.sum(jnp.cumsum(onehot, axis=0) * onehot, axis=1) - 1
    row = flat_route * CAPACITY + rank
    rows = experts * CAPACITY
    picker = (jnp.arange(rows, dtype=jnp.int32)[:, None] == row[None, :]).astype(jnp.bfloat16)
    outgoing = dot(picker, tokens).astype(jnp.bfloat16)
    tiled = (experts, CAPACITY, width // LANES, LANES)
    outgoing, *held = lax.optimization_barrier((outgoing.reshape(tiled), w_gate, w_up, w_down))
    arrived = lax.all_to_all(outgoing, PLANE, 0, 0, tiled=True)
    pieces = list(split_pieces(*held))
    for q in (2, 0, 1):
        pieces[q] = lax.ppermute(pieces[q], "x", cross_pairs(q))
    for q in (3, 2, 0, 1):
        pieces[q] = lax.ppermute(pieces[q], EVERY, pass_pairs(q, experts))
    mid = arrived.reshape(rows, width)
    half = rows // 2

    a, b = mid[:half], mid[half:]
    from_left_a = shift(a, 1)
    from_right_b = shift(b, -1)
    from_left_b = shift(b, 1)
    from_right_a = shift(a, -1)
    far_a = shift(from_left_a, 1)
    far_b = shift(from_right_b, -1)

    kept, edge = multiplicities(partner, own, slots)
    scale = jnp.repeat(kept, hidden // 2)[None, :]
    edge_scale = jnp.repeat(edge, LANES // 2)[None, :]
    outer = ((place == 0) | (place == SPAN - 1)).astype(jnp.int32).reshape(1)
    blocks = [
        jnp.concatenate([far_a, far_b], axis=0),
        jnp.concatenate([from_right_a, from_right_b], axis=0),
        jnp.concatenate([from_left_a, from_left_b], axis=0),
        mid,
    ]
    kept_hidden = [
        (jax.nn.silu(dot(block, w_gate)) * dot(block, w_up) * scale).astype(jnp.bfloat16) for block in blocks
    ]
    tied = lax.optimization_barrier((*pieces, *kept_hidden))
    pieces, kept_hidden = tied[:SPAN], tied[SPAN:]
    edge_into, edge_down = join_pieces(outer, pieces, width)
    down = jnp.concatenate([w_down, edge_down], axis=0)
    quarter = LANES // 2

    def partial(block, own_hidden):
        both = dot(block, edge_into)
        gate = jnp.concatenate([both[:, :quarter], both[:, LANES : LANES + quarter]], axis=1)
        up = jnp.concatenate([both[:, quarter:LANES], both[:, LANES + quarter :]], axis=1)
        edge_hidden = (jax.nn.silu(gate) * up * edge_scale).astype(jnp.bfloat16)
        return dot(jnp.concatenate([own_hidden, edge_hidden], axis=1), down).astype(jnp.bfloat16)

    far, right, left, home = [partial(block, h) for block, h in zip(blocks, kept_hidden)]

    def added(u, v):
        return (u.astype(jnp.float32) + v.astype(jnp.float32)).astype(jnp.bfloat16)

    to_right_a = shift(added(right[:half], shift(far[:half], 1)), 1)
    to_right_b = shift(right[half:], 1)
    to_left_b = shift(added(left[half:], shift(far[half:], -1)), -1)
    to_left_a = shift(left[:half], -1)
    f32 = jnp.float32
    total_a = home[:half].astype(f32) + to_right_a.astype(f32) + to_left_a.astype(f32)
    total_b = home[half:].astype(f32) + to_right_b.astype(f32) + to_left_b.astype(f32)
    total = jnp.concatenate([total_a, total_b], axis=0).astype(jnp.bfloat16)
    returned = lax.all_to_all(total.reshape(tiled), PLANE, 0, 0, tiled=True).reshape(rows, width)
    expert_out = lax.dot_general(picker, returned, (((0,), (0,)), ((), ())), preferred_element_type=f32)
    return (expert_out * gate_prob.reshape(-1)[:, None]).astype(jnp.bfloat16)


def solution(mesh):
    grid = Mesh(mesh.devices.reshape(2, 4, 2, 2, 4), EVERY)
    spec2, spec3 = P(EVERY, None), P(EVERY, None, None)
    return jax.shard_map(
        body,
        mesh=grid,
        in_specs=(spec2, spec2, spec2, spec3, spec3, spec3, P()),
        out_specs=spec2,
        check_vma=False,
    )
```

```python
import jax
import jax.numpy as jnp
from jax import lax
from jax.sharding import Mesh, PartitionSpec as P


SPAN = 4
CAPACITY = 5
PLANE = ("zh", "y", "c", "zl")
EVERY = PLANE + ("x",)
LANES = 128
MIRROR = [(0, 3), (3, 0), (1, 2), (2, 1)]
SIDE = [(0, 1), (1, 0), (2, 3), (3, 2)]
INWARD = [(0, 1), (3, 2)]


def passing(last, first, experts):
    pairs = []
    for e in range(experts):
        pairs.append((SPAN * e + last, SPAN * ((e + 1) % experts) + last))
        pairs.append((SPAN * e + first, SPAN * ((e - 1) % experts) + first))
    return pairs


def multiplicities(partner, own, slots):
    expert, place = own // SPAN, own % SPAN
    start = expert * SPAN
    mine = lax.dynamic_slice_in_dim(partner, start, SPAN, 0)
    kept = jnp.sum((mine == own).astype(jnp.float32), axis=0)
    below = (mine[0] == (start - 1) % slots).astype(jnp.float32)
    above = (mine[SPAN - 1] == (start + SPAN) % slots).astype(jnp.float32)
    sent = jnp.stack([above[0], above[1], below[1], below[0]])
    return kept, sent[place]


def dot(a, b):
    return jnp.dot(a, b, preferred_element_type=jnp.float32)


def body(tokens, route, gate_prob, w_gate, w_up, w_down, partner):
    slots = lax.axis_size(EVERY)
    own = lax.axis_index(EVERY)
    experts = slots // SPAN
    place = lax.axis_index("x")
    width = tokens.shape[1]
    w_gate, w_up, w_down = w_gate[0], w_up[0], w_down[0]
    hidden = w_gate.shape[1]

    flat_route = route.reshape(-1)
    onehot = (flat_route[:, None] == jnp.arange(experts, dtype=jnp.int32)[None, :]).astype(jnp.int32)
    rank = jnp.sum(jnp.cumsum(onehot, axis=0) * onehot, axis=1) - 1
    row = flat_route * CAPACITY + rank
    rows = experts * CAPACITY
    picker = (jnp.arange(rows, dtype=jnp.int32)[:, None] == row[None, :]).astype(jnp.bfloat16)
    outgoing = dot(picker, tokens).astype(jnp.bfloat16)
    tiled = (experts, CAPACITY, width // LANES, LANES)
    outgoing = outgoing.reshape(tiled)
    inner = hidden // 2
    inward_gate = lax.ppermute(w_gate[:, inner:], "x", INWARD)
    inward_up = lax.ppermute(w_up[:, inner:], "x", INWARD)
    arrived = lax.all_to_all(outgoing, PLANE, 0, 0, tiled=True)
    straight, turned = passing(3, 0, experts), passing(2, 1, experts)
    outer_gate = lax.ppermute(w_gate[:, :inner], EVERY, straight)
    outer_up = lax.ppermute(w_up[:, :inner], EVERY, straight)
    outer_down = lax.ppermute(w_down[:inner], EVERY, straight)
    inner_gate = lax.ppermute(inward_gate, EVERY, turned)
    mid = arrived.reshape(rows, width)
    half = rows // 2

    mirror = lax.ppermute(mid, "x", MIRROR)
    side_a = lax.ppermute(mid[:half], "x", SIDE)
    side_b = lax.ppermute(mid[half:], "x", SIDE)
    cut = inner + inner // 2
    inward_down = [lax.ppermute(w, "x", INWARD) for w in (w_down[inner:cut], w_down[cut:])]
    inner_up = lax.ppermute(inward_up, EVERY, turned)
    far_a = lax.ppermute(side_a, "x", MIRROR)
    far_b = lax.ppermute(side_b, "x", MIRROR)
    inner_down = [lax.ppermute(w, EVERY, turned) for w in inward_down]

    kept, edge = multiplicities(partner, own, slots)
    scale = jnp.repeat(kept, inner)[None, :]
    outer = (place == 0) | (place == SPAN - 1)
    edge_into = jnp.concatenate(
        [jnp.where(outer, outer_gate, inner_gate), jnp.where(outer, outer_up, inner_up)], axis=1
    )
    blocks = [
        jnp.concatenate([far_a, far_b], axis=0),
        mirror,
        jnp.concatenate([side_a, side_b], axis=0),
        mid,
    ]

    def hidden_of(block):
        own_hidden = jax.nn.silu(dot(block, w_gate)) * dot(block, w_up) * scale
        both = dot(block, edge_into)
        edge_hidden = jax.nn.silu(both[:, :inner]) * both[:, inner:] * edge
        return jnp.concatenate([own_hidden, edge_hidden], axis=1).astype(jnp.bfloat16)

    tied = lax.optimization_barrier((*inner_down, outer_down, *[hidden_of(block) for block in blocks]))
    inner_down = jnp.concatenate(tied[:2], axis=0)
    down = jnp.concatenate([w_down, jnp.where(outer, tied[2], inner_down)], axis=0)
    far, mirror, side, home = [dot(h, down).astype(jnp.bfloat16) for h in tied[3:]]

    def added(u, v):
        return (u.astype(jnp.float32) + v.astype(jnp.float32)).astype(jnp.bfloat16)

    far_a = lax.ppermute(far[:half], "x", MIRROR)
    far_b = lax.ppermute(far[half:], "x", SIDE)
    mirror_a = lax.ppermute(mirror[:half], "x", MIRROR)
    side_b = lax.ppermute(side[half:], "x", SIDE)
    side_a = lax.ppermute(added(side[:half], far_a), "x", SIDE)
    mirror_b = lax.ppermute(added(mirror[half:], far_b), "x", MIRROR)
    f32 = jnp.float32
    total_a = home[:half].astype(f32) + mirror_a.astype(f32) + side_a.astype(f32)
    total_b = home[half:].astype(f32) + mirror_b.astype(f32) + side_b.astype(f32)
    total = jnp.concatenate([total_a, total_b], axis=0).astype(jnp.bfloat16)
    returned = lax.all_to_all(total.reshape(tiled), PLANE, 0, 0, tiled=True).reshape(rows, width)
    expert_out = lax.dot_general(picker, returned, (((0,), (0,)), ((), ())), preferred_element_type=f32)
    return (expert_out * gate_prob.reshape(-1)[:, None]).astype(jnp.bfloat16)


def solution(mesh):
    grid = Mesh(mesh.devices.reshape(2, 4, 2, 2, 4), EVERY)
    spec2, spec3 = P(EVERY, None), P(EVERY, None, None)
    return jax.shard_map(
        body,
        mesh=grid,
        in_specs=(spec2, spec2, spec2, spec3, spec3, spec3, P()),
        out_specs=spec2,
        check_vma=False,
    )
```

```python
import jax
import jax.numpy as jnp
from jax import lax
from jax.sharding import Mesh, PartitionSpec as P


SPAN = 4
CAPACITY = 5
PLANE = ("zh", "y", "c", "zl")
EVERY = PLANE + ("x",)
LANES = 128
MIRROR = [(0, 3), (3, 0), (1, 2), (2, 1)]
SIDE = [(0, 1), (1, 0), (2, 3), (3, 2)]
INWARD = [(0, 1), (3, 2)]


def passing(last, first, experts):
    pairs = []
    for e in range(experts):
        pairs.append((SPAN * e + last, SPAN * ((e + 1) % experts) + last))
        pairs.append((SPAN * e + first, SPAN * ((e - 1) % experts) + first))
    return pairs


def multiplicities(partner, own, slots):
    expert, place = own // SPAN, own % SPAN
    start = expert * SPAN
    mine = lax.dynamic_slice_in_dim(partner, start, SPAN, 0)
    kept = jnp.sum((mine == own).astype(jnp.float32), axis=0)
    below = (mine[0] == (start - 1) % slots).astype(jnp.float32)
    above = (mine[SPAN - 1] == (start + SPAN) % slots).astype(jnp.float32)
    sent = jnp.stack([above[0], above[1], below[1], below[0]])
    return kept, sent[place]


def dot(a, b):
    return jnp.dot(a, b, preferred_element_type=jnp.float32)


def body(tokens, route, gate_prob, w_gate, w_up, w_down, partner):
    slots = lax.axis_size(EVERY)
    own = lax.axis_index(EVERY)
    experts = slots // SPAN
    place = lax.axis_index("x")
    width = tokens.shape[1]
    w_gate, w_up, w_down = w_gate[0], w_up[0], w_down[0]
    hidden = w_gate.shape[1]

    flat_route = route.reshape(-1)
    onehot = (flat_route[:, None] == jnp.arange(experts, dtype=jnp.int32)[None, :]).astype(jnp.int32)
    rank = jnp.sum(jnp.cumsum(onehot, axis=0) * onehot, axis=1) - 1
    row = flat_route * CAPACITY + rank
    rows = experts * CAPACITY
    picker = (jnp.arange(rows, dtype=jnp.int32)[:, None] == row[None, :]).astype(jnp.bfloat16)
    outgoing = dot(picker, tokens).astype(jnp.bfloat16)
    tiled = (experts, CAPACITY, width // LANES, LANES)
    outgoing = outgoing.reshape(tiled)
    inner = hidden // 2
    first_down = inner + inner * 3 // 4
    straight, turned = passing(3, 0, experts), passing(2, 1, experts)

    def cross(block):
        return lax.ppermute(block, "x", INWARD)

    def over(block, pairs):
        return lax.ppermute(block, "x", pairs)

    inward_down = cross(w_down[inner:first_down])
    inward_gate = cross(w_gate[:, inner:])
    arrived = lax.all_to_all(outgoing, PLANE, 0, 0, tiled=True)
    mid = arrived.reshape(rows, width)

    kept, edge = multiplicities(partner, own, slots)
    scale = jnp.repeat(kept, inner)[None, :]

    def own_hidden(block):
        return (jax.nn.silu(dot(block, w_gate)) * dot(block, w_up) * scale).astype(jnp.bfloat16)

    mirror = over(mid, MIRROR)
    outer_gate = lax.ppermute(w_gate[:, :inner], EVERY, straight)
    outer_up = lax.ppermute(w_up[:, :inner], EVERY, straight)
    outer_down = lax.ppermute(w_down[:inner], EVERY, straight)
    side_a = over(mid[:64], SIDE)
    inward_up = cross(w_up[:, inner:])
    side_b = over(mid[64:128], SIDE)
    side_c = over(mid[128:], SIDE)
    inward_last = cross(w_down[first_down:])
    inner_down = lax.ppermute(inward_down, EVERY, turned)
    inner_gate = lax.ppermute(inward_gate, EVERY, turned)
    far_a = over(side_a, MIRROR)
    inner_up = lax.ppermute(inward_up, EVERY, turned)
    home_own, mirror_own = own_hidden(mid), own_hidden(mirror)
    side_b, home_own, mirror_own = lax.optimization_barrier((side_b, home_own, mirror_own))
    far_b = over(side_b, MIRROR)
    far_c = over(side_c, MIRROR)
    inner_last = lax.ppermute(inward_last, EVERY, turned)

    outer = (place == 0) | (place == SPAN - 1)
    edge_into = jnp.concatenate(
        [jnp.where(outer, outer_gate, inner_gate), jnp.where(outer, outer_up, inner_up)], axis=1
    )
    side = jnp.concatenate([side_a, side_b, side_c], axis=0)
    far = jnp.concatenate([far_a, far_b, far_c], axis=0)

    def full_hidden(block, mine):
        both = dot(block, edge_into)
        edge_hidden = jax.nn.silu(both[:, :inner]) * both[:, inner:] * edge
        return jnp.concatenate([mine, edge_hidden.astype(jnp.bfloat16)], axis=1)

    pairs = ((far, own_hidden(far)), (mirror, mirror_own), (side, own_hidden(side)), (mid, home_own))
    tied = lax.optimization_barrier((inner_down, inner_last, outer_down, *[full_hidden(*p) for p in pairs]))
    edge_down = jnp.where(outer, tied[2], jnp.concatenate(tied[:2], axis=0))
    down = jnp.concatenate([w_down, edge_down], axis=0)
    far, mirror, side, home = [dot(h, down).astype(jnp.bfloat16) for h in tied[3:]]

    def added(u, v):
        return (u.astype(jnp.float32) + v.astype(jnp.float32)).astype(jnp.bfloat16)

    f32 = jnp.float32
    half = rows // 2
    upper, lower = slice(None, half), slice(half, None)
    outs = []
    for lo, hi in ((0, 4096), (4096, width)):
        cols = slice(lo, hi)
        far_a = over(far[upper, cols], MIRROR)
        far_b = over(far[lower, cols], SIDE)
        mirror_a = over(mirror[upper, cols], MIRROR)
        side_b = over(side[lower, cols], SIDE)
        side_a = over(added(side[upper, cols], far_a), SIDE)
        mirror_b = over(added(mirror[lower, cols], far_b), MIRROR)
        total_a = home[upper, cols].astype(f32) + mirror_a.astype(f32) + side_a.astype(f32)
        total_b = home[lower, cols].astype(f32) + mirror_b.astype(f32) + side_b.astype(f32)
        total = jnp.concatenate([total_a, total_b], axis=0).astype(jnp.bfloat16)
        total = total.reshape(experts, CAPACITY, (hi - lo) // LANES, LANES)
        returned = lax.all_to_all(total, PLANE, 0, 0, tiled=True).reshape(rows, hi - lo)
        expert_out = lax.dot_general(picker, returned, (((0,), (0,)), ((), ())), preferred_element_type=f32)
        outs.append((expert_out * gate_prob.reshape(-1)[:, None]).astype(jnp.bfloat16))
    return jnp.concatenate(outs, axis=1)


def solution(mesh):
    grid = Mesh(mesh.devices.reshape(2, 4, 2, 2, 4), EVERY)
    spec2, spec3 = P(EVERY, None), P(EVERY, None, None)
    return jax.shard_map(
        body,
        mesh=grid,
        in_specs=(spec2, spec2, spec2, spec3, spec3, spec3, P()),
        out_specs=spec2,
        check_vma=False,
    )
```

```python
import jax
import jax.numpy as jnp
from jax import lax
from jax.sharding import Mesh, PartitionSpec as P


SPAN = 4
CAPACITY = 5
PLANE = ("zh", "y", "c", "zl")
EVERY = PLANE + ("x",)
LANES = 128
MIRROR = [(0, 3), (3, 0), (1, 2), (2, 1)]
SIDE = [(0, 1), (1, 0), (2, 3), (3, 2)]
INWARD = [(0, 1), (3, 2)]


def passing(last, first, experts):
    pairs = []
    for e in range(experts):
        pairs.append((SPAN * e + last, SPAN * ((e + 1) % experts) + last))
        pairs.append((SPAN * e + first, SPAN * ((e - 1) % experts) + first))
    return pairs


def multiplicities(partner, own, slots):
    expert, place = own // SPAN, own % SPAN
    start = expert * SPAN
    mine = lax.dynamic_slice_in_dim(partner, start, SPAN, 0)
    kept = jnp.sum((mine == own).astype(jnp.float32), axis=0)
    below = (mine[0] == (start - 1) % slots).astype(jnp.float32)
    above = (mine[SPAN - 1] == (start + SPAN) % slots).astype(jnp.float32)
    sent = jnp.stack([above[0], above[1], below[1], below[0]])
    return kept, sent[place]


def dot(a, b):
    return jnp.dot(a, b, preferred_element_type=jnp.float32)


def body(tokens, route, gate_prob, w_gate, w_up, w_down, partner):
    slots = lax.axis_size(EVERY)
    own = lax.axis_index(EVERY)
    experts = slots // SPAN
    place = lax.axis_index("x")
    width = tokens.shape[1]
    w_gate, w_up, w_down = w_gate[0], w_up[0], w_down[0]
    hidden = w_gate.shape[1]

    flat_route = route.reshape(-1)
    onehot = (flat_route[:, None] == jnp.arange(experts, dtype=jnp.int32)[None, :]).astype(jnp.int32)
    rank = jnp.sum(jnp.cumsum(onehot, axis=0) * onehot, axis=1) - 1
    row = flat_route * CAPACITY + rank
    rows = experts * CAPACITY
    picker = (jnp.arange(rows, dtype=jnp.int32)[:, None] == row[None, :]).astype(jnp.bfloat16)
    outgoing = dot(picker, tokens).astype(jnp.bfloat16)
    tiled = (experts, CAPACITY, width // LANES, LANES)
    outgoing = outgoing.reshape(tiled)
    inner = hidden // 2
    first_down = inner + inner * 3 // 4
    straight, turned = passing(3, 0, experts), passing(2, 1, experts)

    def cross(block):
        return lax.ppermute(block, "x", INWARD)

    def over(block, pairs):
        return lax.ppermute(block, "x", pairs)

    inward_down = cross(w_down[inner:first_down])
    inward_gate = cross(w_gate[:, inner:])
    inward_up = cross(w_up[:, inner:])
    arrived = lax.all_to_all(outgoing, PLANE, 0, 0, tiled=True)
    mid = arrived.reshape(rows, width)

    kept, edge = multiplicities(partner, own, slots)
    scale = jnp.repeat(kept, inner)[None, :]

    def own_hidden(block):
        return (jax.nn.silu(dot(block, w_gate)) * dot(block, w_up) * scale).astype(jnp.bfloat16)

    mirror = over(mid, MIRROR)
    outer_gate = lax.ppermute(w_gate[:, :inner], EVERY, straight)
    outer_up = lax.ppermute(w_up[:, :inner], EVERY, straight)
    outer_down = lax.ppermute(w_down[:inner], EVERY, straight)
    side_a = over(mid[:64], SIDE)
    side_b = over(mid[64:128], SIDE)
    side_c = over(mid[128:], SIDE)
    inward_last = cross(w_down[first_down:])
    inner_down = lax.ppermute(inward_down, EVERY, turned)
    inner_gate = lax.ppermute(inward_gate, EVERY, turned)
    far_a = over(side_a, MIRROR)
    inner_up = lax.ppermute(inward_up, EVERY, turned)
    home_own, mirror_own = own_hidden(mid), own_hidden(mirror)
    side_b, home_own, mirror_own = lax.optimization_barrier((side_b, home_own, mirror_own))
    far_b = over(side_b, MIRROR)
    far_c = over(side_c, MIRROR)
    inner_last = lax.ppermute(inward_last, EVERY, turned)

    outer = (place == 0) | (place == SPAN - 1)
    edge_gate = jnp.where(outer, outer_gate, inner_gate)
    edge_up = jnp.where(outer, outer_up, inner_up)
    edge_into = jnp.concatenate([edge_gate, edge_up], axis=1)
    side = jnp.concatenate([side_a, side_b, side_c], axis=0)
    far = jnp.concatenate([far_a, far_b, far_c], axis=0)

    def full_hidden(block, mine):
        both = dot(block, edge_into)
        edge_hidden = jax.nn.silu(both[:, :inner]) * both[:, inner:] * edge
        return jnp.concatenate([mine, edge_hidden.astype(jnp.bfloat16)], axis=1)

    pairs = ((far, own_hidden(far)), (mirror, mirror_own), (side, own_hidden(side)), (mid, home_own))
    tied = lax.optimization_barrier((inner_down, inner_last, outer_down, *[full_hidden(*p) for p in pairs]))
    edge_down = jnp.where(outer, tied[2], jnp.concatenate(tied[:2], axis=0))
    down = jnp.concatenate([w_down, edge_down], axis=0)
    far = dot(tied[3], down).astype(jnp.bfloat16)
    far, *rest = lax.optimization_barrier((far, *tied[4:]))
    mirror, side, home = [dot(h, down).astype(jnp.bfloat16) for h in rest]

    def added(u, v):
        return (u.astype(jnp.float32) + v.astype(jnp.float32)).astype(jnp.bfloat16)

    f32 = jnp.float32
    half = rows // 2
    upper, lower = slice(None, half), slice(half, None)
    outs = []
    for lo, hi in ((0, 4096), (4096, width)):
        cols = slice(lo, hi)
        far_a = over(far[upper, cols], MIRROR)
        far_b = over(far[lower, cols], SIDE)
        mirror_a = over(mirror[upper, cols], MIRROR)
        side_b = over(side[lower, cols], SIDE)
        side_a = added(side[upper, cols], far_a)
        mirror_b = added(mirror[lower, cols], far_b)
        side_a = over(side_a, SIDE)
        mirror_b = over(mirror_b, MIRROR)
        total_a = home[upper, cols].astype(f32) + mirror_a.astype(f32) + side_a.astype(f32)
        total_b = home[lower, cols].astype(f32) + mirror_b.astype(f32) + side_b.astype(f32)
        total = jnp.concatenate([total_a, total_b], axis=0).astype(jnp.bfloat16)
        total = total.reshape(experts, CAPACITY, (hi - lo) // LANES, LANES)
        returned = lax.all_to_all(total, PLANE, 0, 0, tiled=True).reshape(rows, hi - lo)
        expert_out = lax.dot_general(picker, returned, (((0,), (0,)), ((), ())), preferred_element_type=f32)
        outs.append((expert_out * gate_prob.reshape(-1)[:, None]).astype(jnp.bfloat16))
    return jnp.concatenate(outs, axis=1)


def solution(mesh):
    grid = Mesh(mesh.devices.reshape(2, 4, 2, 2, 4), EVERY)
    spec2, spec3 = P(EVERY, None), P(EVERY, None, None)
    return jax.shard_map(
        body,
        mesh=grid,
        in_specs=(spec2, spec2, spec2, spec3, spec3, spec3, P()),
        out_specs=spec2,
        check_vma=False,
    )
```

```python
import jax
import jax.numpy as jnp
from jax import lax
from jax.sharding import Mesh, PartitionSpec as P


SPAN = 4
CAPACITY = 5
PLANE = ("zh", "y", "c", "zl")
EVERY = PLANE + ("x",)
LANES = 128
MIRROR = [(0, 3), (3, 0), (1, 2), (2, 1)]
SIDE = [(0, 1), (1, 0), (2, 3), (3, 2)]
INWARD = [(0, 1), (3, 2)]


def passing(last, first, experts):
    pairs = []
    for e in range(experts):
        pairs.append((SPAN * e + last, SPAN * ((e + 1) % experts) + last))
        pairs.append((SPAN * e + first, SPAN * ((e - 1) % experts) + first))
    return pairs


def multiplicities(partner, own, slots):
    expert, place = own // SPAN, own % SPAN
    start = expert * SPAN
    mine = lax.dynamic_slice_in_dim(partner, start, SPAN, 0)
    kept = jnp.sum((mine == own).astype(jnp.float32), axis=0)
    below = (mine[0] == (start - 1) % slots).astype(jnp.float32)
    above = (mine[SPAN - 1] == (start + SPAN) % slots).astype(jnp.float32)
    sent = jnp.stack([above[0], above[1], below[1], below[0]])
    return kept, sent[place]


def dot(a, b):
    return jnp.dot(a, b, preferred_element_type=jnp.float32)


def body(tokens, route, gate_prob, w_gate, w_up, w_down, partner):
    slots = lax.axis_size(EVERY)
    own = lax.axis_index(EVERY)
    experts = slots // SPAN
    place = lax.axis_index("x")
    width = tokens.shape[1]
    w_gate, w_up, w_down = w_gate[0], w_up[0], w_down[0]
    hidden = w_gate.shape[1]

    flat_route = route.reshape(-1)
    onehot = (flat_route[:, None] == jnp.arange(experts, dtype=jnp.int32)[None, :]).astype(jnp.int32)
    rank = jnp.sum(jnp.cumsum(onehot, axis=0) * onehot, axis=1) - 1
    row = flat_route * CAPACITY + rank
    rows = experts * CAPACITY
    picker = (jnp.arange(rows, dtype=jnp.int32)[:, None] == row[None, :]).astype(jnp.bfloat16)
    outgoing = dot(picker, tokens).astype(jnp.bfloat16)
    tiled = (experts, CAPACITY, width // LANES, LANES)
    outgoing = outgoing.reshape(tiled)
    inner = hidden // 2
    first_down = inner + inner * 3 // 4
    straight, turned = passing(3, 0, experts), passing(2, 1, experts)

    def cross(block):
        return lax.ppermute(block, "x", INWARD)

    def over(block, pairs):
        return lax.ppermute(block, "x", pairs)

    inward_down = cross(w_down[inner:first_down])
    inward_gate = cross(w_gate[:, inner:])
    inward_up = cross(w_up[:, inner:])
    arrived = lax.all_to_all(outgoing, PLANE, 0, 0, tiled=True)
    mid = arrived.reshape(rows, width)

    kept, edge = multiplicities(partner, own, slots)
    scale = jnp.repeat(kept, inner)[None, :]

    def own_hidden(block):
        return (jax.nn.silu(dot(block, w_gate)) * dot(block, w_up) * scale).astype(jnp.bfloat16)

    mirror = over(mid, MIRROR)
    outer_gate = lax.ppermute(w_gate[:, :inner], EVERY, straight)
    outer_up = lax.ppermute(w_up[:, :inner], EVERY, straight)
    outer_down = lax.ppermute(w_down[:inner], EVERY, straight)
    side_a = over(mid[:64], SIDE)
    side_b = over(mid[64:128], SIDE)
    side_c = over(mid[128:], SIDE)
    inward_last = cross(w_down[first_down:])
    inner_down = lax.ppermute(inward_down, EVERY, turned)
    inner_gate = lax.ppermute(inward_gate, EVERY, turned)
    far_a = over(side_a, MIRROR)
    inner_up = lax.ppermute(inward_up, EVERY, turned)
    home_own, mirror_own = own_hidden(mid), own_hidden(mirror)
    side_b, home_own, mirror_own = lax.optimization_barrier((side_b, home_own, mirror_own))
    far_b = over(side_b, MIRROR)
    far_c = over(side_c, MIRROR)
    inner_last = lax.ppermute(inward_last, EVERY, turned)

    outer = (place == 0) | (place == SPAN - 1)
    edge_gate = jnp.where(outer, outer_gate, inner_gate)
    edge_up = jnp.where(outer, outer_up, inner_up)
    edge_into = jnp.concatenate([edge_gate, edge_up], axis=1)
    side = jnp.concatenate([side_a, side_b, side_c], axis=0)
    far = jnp.concatenate(lax.optimization_barrier((far_a, far_b, far_c)), axis=0)

    def full_hidden(block, mine):
        both = dot(block, edge_into)
        edge_hidden = jax.nn.silu(both[:, :inner]) * both[:, inner:] * edge
        return jnp.concatenate([mine, edge_hidden.astype(jnp.bfloat16)], axis=1)

    pairs = ((far, own_hidden(far)), (mirror, mirror_own), (side, own_hidden(side)))
    tied = lax.optimization_barrier((inner_down, inner_last, outer_down, *[full_hidden(*p) for p in pairs]))
    edge_down = jnp.where(outer, tied[2], jnp.concatenate(tied[:2], axis=0))
    down = jnp.concatenate([w_down, edge_down], axis=0)
    far = dot(tied[3], down).astype(jnp.bfloat16)
    far, mirror, side, mid, home_own = lax.optimization_barrier((far, *tied[4:], mid, home_own))
    mirror, side, home = [dot(h, down).astype(jnp.bfloat16) for h in (mirror, side, full_hidden(mid, home_own))]

    def added(u, v):
        return (u.astype(jnp.float32) + v.astype(jnp.float32)).astype(jnp.bfloat16)

    f32 = jnp.float32
    half = rows // 2
    upper, lower = slice(None, half), slice(half, None)
    result = jnp.zeros(tokens.shape, jnp.bfloat16)
    for lo, hi in ((0, 4096), (4096, width)):
        cols = slice(lo, hi)
        far_a = over(far[upper, cols], MIRROR)
        far_b = over(far[lower, cols], SIDE)
        mirror_a = over(mirror[upper, cols], MIRROR)
        side_b = over(side[lower, cols], SIDE)
        side_a = added(side[upper, cols], far_a)
        mirror_b = added(mirror[lower, cols], far_b)
        side_a = over(side_a, SIDE)
        mirror_b = over(mirror_b, MIRROR)
        total_a = home[upper, cols].astype(f32) + mirror_a.astype(f32) + side_a.astype(f32)
        total_b = home[lower, cols].astype(f32) + mirror_b.astype(f32) + side_b.astype(f32)
        total = jnp.concatenate([total_a, total_b], axis=0).astype(jnp.bfloat16)
        total = total.reshape(experts, CAPACITY, (hi - lo) // LANES, LANES)
        returned = lax.all_to_all(total, PLANE, 0, 0, tiled=True).reshape(rows, hi - lo)
        expert_out = lax.dot_general(picker, returned, (((0,), (0,)), ((), ())), preferred_element_type=f32)
        mixed = (expert_out * gate_prob.reshape(-1)[:, None]).astype(jnp.bfloat16)
        result = lax.dynamic_update_slice(result, mixed, (0, lo))
    return result


def solution(mesh):
    grid = Mesh(mesh.devices.reshape(2, 4, 2, 2, 4), EVERY)
    spec2, spec3 = P(EVERY, None), P(EVERY, None, None)
    return jax.shard_map(
        body,
        mesh=grid,
        in_specs=(spec2, spec2, spec2, spec3, spec3, spec3, P()),
        out_specs=spec2,
        check_vma=False,
    )
```

```python
import jax
import jax.numpy as jnp
from jax import lax
from jax.sharding import Mesh, PartitionSpec as P


SPAN = 4
CAPACITY = 5
PLANE = ("zh", "y", "c", "zl")
EVERY = PLANE + ("x",)
LANES = 128
MIRROR = [(0, 3), (3, 0), (1, 2), (2, 1)]
SIDE = [(0, 1), (1, 0), (2, 3), (3, 2)]
INWARD = [(0, 1), (3, 2)]


def passing(last, first, experts):
    pairs = []
    for e in range(experts):
        pairs.append((SPAN * e + last, SPAN * ((e + 1) % experts) + last))
        pairs.append((SPAN * e + first, SPAN * ((e - 1) % experts) + first))
    return pairs


def multiplicities(partner, own, slots):
    expert, place = own // SPAN, own % SPAN
    start = expert * SPAN
    mine = lax.dynamic_slice_in_dim(partner, start, SPAN, 0)
    kept = jnp.sum((mine == own).astype(jnp.float32), axis=0)
    below = (mine[0] == (start - 1) % slots).astype(jnp.float32)
    above = (mine[SPAN - 1] == (start + SPAN) % slots).astype(jnp.float32)
    sent = jnp.stack([above[0], above[1], below[1], below[0]])
    return kept, sent[place]


def dot(a, b):
    return jnp.dot(a, b, preferred_element_type=jnp.float32)


def body(tokens, route, gate_prob, w_gate, w_up, w_down, partner):
    slots = lax.axis_size(EVERY)
    own = lax.axis_index(EVERY)
    experts = slots // SPAN
    place = lax.axis_index("x")
    width = tokens.shape[1]
    w_gate, w_up, w_down = w_gate[0], w_up[0], w_down[0]
    hidden = w_gate.shape[1]

    flat_route = route.reshape(-1)
    onehot = (flat_route[:, None] == jnp.arange(experts, dtype=jnp.int32)[None, :]).astype(jnp.int32)
    rank = jnp.sum(jnp.cumsum(onehot, axis=0) * onehot, axis=1) - 1
    row = flat_route * CAPACITY + rank
    rows = experts * CAPACITY
    picker = (jnp.arange(rows, dtype=jnp.int32)[:, None] == row[None, :]).astype(jnp.bfloat16)
    outgoing = dot(picker, tokens).astype(jnp.bfloat16)
    tiled = (experts, CAPACITY, width // LANES, LANES)
    outgoing = outgoing.reshape(tiled)
    inner = hidden // 2
    first_down = inner + inner * 3 // 4
    straight, turned = passing(3, 0, experts), passing(2, 1, experts)

    def cross(block):
        return lax.ppermute(block, "x", INWARD)

    def over(block, pairs):
        return lax.ppermute(block, "x", pairs)

    inward_down = cross(w_down[inner:first_down])
    inward_gate = cross(w_gate[:, inner:])
    inward_up = cross(w_up[:, inner:])
    arrived = lax.all_to_all(outgoing, PLANE, 0, 0, tiled=True)
    outer_early = lax.ppermute(w_down[: inner // 2], EVERY, straight)
    mid = arrived.reshape(rows, width)

    kept, edge = multiplicities(partner, own, slots)
    scale = jnp.repeat(kept, inner)[None, :]

    def own_hidden(block):
        return (jax.nn.silu(dot(block, w_gate)) * dot(block, w_up) * scale).astype(jnp.bfloat16)

    mirror = over(mid, MIRROR)
    outer_gate = lax.ppermute(w_gate[:, :inner], EVERY, straight)
    outer_up = lax.ppermute(w_up[:, :inner], EVERY, straight)
    outer_late = lax.ppermute(w_down[inner // 2 : inner], EVERY, straight)
    side_a = over(mid[:64], SIDE)
    side_b = over(mid[64:128], SIDE)
    side_c = over(mid[128:], SIDE)
    inward_last = cross(w_down[first_down:])
    inner_down = lax.ppermute(inward_down, EVERY, turned)
    inner_gate = lax.ppermute(inward_gate, EVERY, turned)
    far_a = over(side_a, MIRROR)
    inner_up = lax.ppermute(inward_up, EVERY, turned)
    home_own, mirror_own = own_hidden(mid), own_hidden(mirror)
    side_b, home_own, mirror_own = lax.optimization_barrier((side_b, home_own, mirror_own))
    far_b = over(side_b, MIRROR)
    far_c = over(side_c, MIRROR)
    inner_last = lax.ppermute(inward_last, EVERY, turned)

    outer = (place == 0) | (place == SPAN - 1)
    edge_gate = jnp.where(outer, outer_gate, inner_gate)
    edge_up = jnp.where(outer, outer_up, inner_up)
    edge_into = jnp.concatenate([edge_gate, edge_up], axis=1)
    side = jnp.concatenate([side_a, side_b, side_c], axis=0)
    far = jnp.concatenate(lax.optimization_barrier((far_a, far_b, far_c)), axis=0)

    def full_hidden(block, mine):
        both = dot(block, edge_into)
        edge_hidden = jax.nn.silu(both[:, :inner]) * both[:, inner:] * edge
        return jnp.concatenate([mine, edge_hidden.astype(jnp.bfloat16)], axis=1)

    pairs = ((far, own_hidden(far)), (mirror, mirror_own), (side, own_hidden(side)))
    downs = (outer_early, outer_late, inner_down, inner_last)
    tied = lax.optimization_barrier((*downs, *[full_hidden(*p) for p in pairs]))
    outer_down, inner_down = jnp.concatenate(tied[:2], axis=0), jnp.concatenate(tied[2:4], axis=0)
    down = jnp.concatenate([w_down, jnp.where(outer, outer_down, inner_down)], axis=0)
    far = dot(tied[4], down).astype(jnp.bfloat16)
    far, mirror, side, mid, home_own = lax.optimization_barrier((far, *tied[5:], mid, home_own))
    mirror, side = [dot(h, down).astype(jnp.bfloat16) for h in (mirror, side)]
    home = dot(full_hidden(mid, home_own), down).astype(jnp.bfloat16)

    def added(u, v):
        return (u.astype(jnp.float32) + v.astype(jnp.float32)).astype(jnp.bfloat16)

    f32 = jnp.float32
    half = rows // 2
    upper, lower = slice(None, half), slice(half, None)
    result = jnp.zeros(tokens.shape, jnp.bfloat16)
    for lo, hi in ((0, 4096), (4096, width)):
        cols = slice(lo, hi)
        far_a = over(far[upper, cols], MIRROR)
        far_b = over(far[lower, cols], SIDE)
        mirror_a = over(mirror[upper, cols], MIRROR)
        side_b = over(side[lower, cols], SIDE)
        side_a = added(side[upper, cols], far_a)
        mirror_b = added(mirror[lower, cols], far_b)
        side_a = over(side_a, SIDE)
        mirror_b = over(mirror_b, MIRROR)
        total_a = home[upper, cols].astype(f32) + mirror_a.astype(f32) + side_a.astype(f32)
        total_b = home[lower, cols].astype(f32) + mirror_b.astype(f32) + side_b.astype(f32)
        total = jnp.concatenate([total_a, total_b], axis=0).astype(jnp.bfloat16)
        total = total.reshape(experts, CAPACITY, (hi - lo) // LANES, LANES)
        returned = lax.all_to_all(total, PLANE, 0, 0, tiled=True).reshape(rows, hi - lo)
        expert_out = lax.dot_general(picker, returned, (((0,), (0,)), ((), ())), preferred_element_type=f32)
        mixed = (expert_out * gate_prob.reshape(-1)[:, None]).astype(jnp.bfloat16)
        result = lax.dynamic_update_slice(result, mixed, (0, lo))
    return result


def solution(mesh):
    grid = Mesh(mesh.devices.reshape(2, 4, 2, 2, 4), EVERY)
    spec2, spec3 = P(EVERY, None), P(EVERY, None, None)
    return jax.shard_map(
        body,
        mesh=grid,
        in_specs=(spec2, spec2, spec2, spec3, spec3, spec3, P()),
        out_specs=spec2,
        check_vma=False,
    )
```

```python
import jax
import jax.numpy as jnp
from jax import lax
from jax.sharding import Mesh, PartitionSpec as P


SPAN = 4
CAPACITY = 5
PLANE = ("zh", "y", "c", "zl")
EVERY = PLANE + ("x",)
LANES = 128
MIRROR = [(0, 3), (3, 0), (1, 2), (2, 1)]
SIDE = [(0, 1), (1, 0), (2, 3), (3, 2)]
INWARD = [(0, 1), (3, 2)]


def passing(last, first, experts):
    pairs = []
    for e in range(experts):
        pairs.append((SPAN * e + last, SPAN * ((e + 1) % experts) + last))
        pairs.append((SPAN * e + first, SPAN * ((e - 1) % experts) + first))
    return pairs


def multiplicities(partner, own, slots):
    expert, place = own // SPAN, own % SPAN
    start = expert * SPAN
    mine = lax.dynamic_slice_in_dim(partner, start, SPAN, 0)
    kept = jnp.sum((mine == own).astype(jnp.float32), axis=0)
    below = (mine[0] == (start - 1) % slots).astype(jnp.float32)
    above = (mine[SPAN - 1] == (start + SPAN) % slots).astype(jnp.float32)
    sent = jnp.stack([above[0], above[1], below[1], below[0]])
    return kept, sent[place]


def dot(a, b):
    return jnp.dot(a, b, preferred_element_type=jnp.float32)


def body(tokens, route, gate_prob, w_gate, w_up, w_down, partner):
    slots = lax.axis_size(EVERY)
    own = lax.axis_index(EVERY)
    experts = slots // SPAN
    place = lax.axis_index("x")
    width = tokens.shape[1]
    w_gate, w_up, w_down = w_gate[0], w_up[0], w_down[0]
    hidden = w_gate.shape[1]

    flat_route = route.reshape(-1)
    onehot = (flat_route[:, None] == jnp.arange(experts, dtype=jnp.int32)[None, :]).astype(jnp.int32)
    rank = jnp.sum(jnp.cumsum(onehot, axis=0) * onehot, axis=1) - 1
    row = flat_route * CAPACITY + rank
    rows = experts * CAPACITY
    picker = (jnp.arange(rows, dtype=jnp.int32)[:, None] == row[None, :]).astype(jnp.bfloat16)
    outgoing = dot(picker, tokens).astype(jnp.bfloat16)
    tiled = (experts, CAPACITY, width // LANES, LANES)
    outgoing = outgoing.reshape(tiled)
    inner = hidden // 2
    first_down = inner + 104
    straight, turned = passing(3, 0, experts), passing(2, 1, experts)

    def cross(block):
        return lax.ppermute(block, "x", INWARD)

    def over(block, pairs):
        return lax.ppermute(block, "x", pairs)

    inward_down = cross(w_down[inner:first_down])
    inward_gate = cross(w_gate[:, inner:])
    arrived = lax.all_to_all(outgoing, PLANE, 0, 0, tiled=True)
    outer_early = lax.ppermute(w_down[: inner // 2], EVERY, straight)
    mid = arrived.reshape(rows, width)

    kept, edge = multiplicities(partner, own, slots)
    scale = jnp.repeat(kept, inner)[None, :]

    def own_hidden(block):
        return (jax.nn.silu(dot(block, w_gate)) * dot(block, w_up) * scale).astype(jnp.bfloat16)

    mirror = over(mid, MIRROR)
    outer_gate = lax.ppermute(w_gate[:, :inner], EVERY, straight)
    outer_up = lax.ppermute(w_up[:, :inner], EVERY, straight)
    outer_late = lax.ppermute(w_down[inner // 2 : inner], EVERY, straight)
    side_a = over(mid[:64], SIDE)
    inward_up = cross(w_up[:, inner:])
    side_b = over(mid[64:112], SIDE)
    side_c = over(mid[112:], SIDE)
    inward_last = cross(w_down[first_down:])
    inner_down = lax.ppermute(inward_down, EVERY, turned)
    inner_gate = lax.ppermute(inward_gate, EVERY, turned)
    far_a = over(side_a, MIRROR)
    inner_up = lax.ppermute(inward_up, EVERY, turned)
    home_own, mirror_own = own_hidden(mid), own_hidden(mirror)
    side_b, home_own, mirror_own = lax.optimization_barrier((side_b, home_own, mirror_own))
    far_b = over(side_b, MIRROR)
    far_c = over(side_c, MIRROR)
    inner_last = lax.ppermute(inward_last, EVERY, turned)

    outer = (place == 0) | (place == SPAN - 1)
    edge_gate = jnp.where(outer, outer_gate, inner_gate)
    edge_up = jnp.where(outer, outer_up, inner_up)
    edge_into = jnp.concatenate([edge_gate, edge_up], axis=1)
    side = jnp.concatenate([side_a, side_b, side_c], axis=0)
    far = jnp.concatenate(lax.optimization_barrier((far_a, far_b, far_c)), axis=0)

    def full_hidden(block, mine):
        both = dot(block, edge_into)
        edge_hidden = jax.nn.silu(both[:, :inner]) * both[:, inner:] * edge
        return jnp.concatenate([mine, edge_hidden.astype(jnp.bfloat16)], axis=1)

    pairs = ((far, own_hidden(far)), (mirror, mirror_own), (side, own_hidden(side)))
    downs = (outer_early, outer_late, inner_down, inner_last)
    tied = lax.optimization_barrier((*downs, *[full_hidden(*p) for p in pairs]))
    outer_down, inner_down = jnp.concatenate(tied[:2], axis=0), jnp.concatenate(tied[2:4], axis=0)
    down = jnp.concatenate([w_down, jnp.where(outer, outer_down, inner_down)], axis=0)
    far = dot(tied[4], down).astype(jnp.bfloat16)
    far, mirror, side, mid, home_own = lax.optimization_barrier((far, *tied[5:], mid, home_own))
    mirror, side = [dot(h, down).astype(jnp.bfloat16) for h in (mirror, side)]
    home = dot(full_hidden(mid, home_own), down).astype(jnp.bfloat16)

    def added(u, v):
        return (u.astype(jnp.float32) + v.astype(jnp.float32)).astype(jnp.bfloat16)

    f32 = jnp.float32
    half = rows // 2
    upper, lower = slice(None, half), slice(half, None)
    result = None
    for lo, hi in ((0, 4096), (4096, width)):
        cols = slice(lo, hi)
        far_a = over(far[upper, cols], MIRROR)
        far_b = over(far[lower, cols], SIDE)
        mirror_a = over(mirror[upper, cols], MIRROR)
        side_b = over(side[lower, cols], SIDE)
        side_a = added(side[upper, cols], far_a)
        mirror_b = added(mirror[lower, cols], far_b)
        side_a = over(side_a, SIDE)
        mirror_b = over(mirror_b, MIRROR)
        total_a = home[upper, cols].astype(f32) + mirror_a.astype(f32) + side_a.astype(f32)
        total_b = home[lower, cols].astype(f32) + mirror_b.astype(f32) + side_b.astype(f32)
        total = jnp.concatenate([total_a, total_b], axis=0).astype(jnp.bfloat16)
        total = total.reshape(experts, CAPACITY, (hi - lo) // LANES, LANES)
        returned = lax.all_to_all(total, PLANE, 0, 0, tiled=True).reshape(rows, hi - lo)
        expert_out = lax.dot_general(picker, returned, (((0,), (0,)), ((), ())), preferred_element_type=f32)
        mixed = (expert_out * gate_prob.reshape(-1)[:, None]).astype(jnp.bfloat16)
        if result is None:
            result = lax.optimization_barrier(jnp.pad(mixed, ((0, 0), (0, width - hi))))
        else:
            result = lax.dynamic_update_slice(result, mixed, (0, lo))
    return result


def solution(mesh):
    grid = Mesh(mesh.devices.reshape(2, 4, 2, 2, 4), EVERY)
    spec2, spec3 = P(EVERY, None), P(EVERY, None, None)
    return jax.shard_map(
        body,
        mesh=grid,
        in_specs=(spec2, spec2, spec2, spec3, spec3, spec3, P()),
        out_specs=spec2,
        check_vma=False,
    )
```

```python
import jax
import jax.numpy as jnp
from jax import lax
from jax.sharding import Mesh, PartitionSpec as P


SPAN = 4
CAPACITY = 5
PLANE = ("zh", "y", "c", "zl")
EVERY = PLANE + ("x",)
LANES = 128
MIRROR = [(0, 3), (3, 0), (1, 2), (2, 1)]
SIDE = [(0, 1), (1, 0), (2, 3), (3, 2)]
INWARD = [(0, 1), (3, 2)]


def passing(last, first, experts):
    pairs = []
    for e in range(experts):
        pairs.append((SPAN * e + last, SPAN * ((e + 1) % experts) + last))
        pairs.append((SPAN * e + first, SPAN * ((e - 1) % experts) + first))
    return pairs


def multiplicities(partner, own, slots):
    expert, place = own // SPAN, own % SPAN
    start = expert * SPAN
    mine = lax.dynamic_slice_in_dim(partner, start, SPAN, 0)
    kept = jnp.sum((mine == own).astype(jnp.float32), axis=0)
    below = (mine[0] == (start - 1) % slots).astype(jnp.float32)
    above = (mine[SPAN - 1] == (start + SPAN) % slots).astype(jnp.float32)
    sent = jnp.stack([above[0], above[1], below[1], below[0]])
    return kept, sent[place]


def dot(a, b):
    return jnp.dot(a, b, preferred_element_type=jnp.float32)


def body(tokens, route, gate_prob, w_gate, w_up, w_down, partner):
    slots = lax.axis_size(EVERY)
    own = lax.axis_index(EVERY)
    experts = slots // SPAN
    place = lax.axis_index("x")
    width = tokens.shape[1]
    w_gate, w_up, w_down = w_gate[0], w_up[0], w_down[0]
    hidden = w_gate.shape[1]

    flat_route = route.reshape(-1)
    onehot = (flat_route[:, None] == jnp.arange(experts, dtype=jnp.int32)[None, :]).astype(jnp.int32)
    rank = jnp.sum(jnp.cumsum(onehot, axis=0) * onehot, axis=1) - 1
    row = flat_route * CAPACITY + rank
    rows = experts * CAPACITY
    picker = (jnp.arange(rows, dtype=jnp.int32)[:, None] == row[None, :]).astype(jnp.bfloat16)
    outgoing = dot(picker, tokens).astype(jnp.bfloat16)
    tiled = (experts, CAPACITY, width // LANES, LANES)
    outgoing = outgoing.reshape(tiled)
    inner = hidden // 2
    first_down = inner + 104
    straight, turned = passing(3, 0, experts), passing(2, 1, experts)

    def cross(block):
        return lax.ppermute(block, "x", INWARD)

    def over(block, pairs):
        return lax.ppermute(block, "x", pairs)

    inward_down = cross(w_down[inner:first_down])
    inward_gate = cross(w_gate[:, inner:])
    inward_up = cross(w_up[:, inner:])
    arrived = lax.all_to_all(outgoing, PLANE, 0, 0, tiled=True)
    mid = arrived.reshape(rows, width)

    kept, edge = multiplicities(partner, own, slots)
    scale = jnp.repeat(kept, inner)[None, :]

    def own_hidden(block):
        return (jax.nn.silu(dot(block, w_gate)) * dot(block, w_up) * scale).astype(jnp.bfloat16)

    mirror = over(mid, MIRROR)
    outer_gate = lax.ppermute(w_gate[:, :inner], EVERY, straight)
    outer_up = lax.ppermute(w_up[:, :inner], EVERY, straight)
    outer_down = lax.ppermute(w_down[:inner], EVERY, straight)
    side_a = over(mid[:56], SIDE)
    side_b = over(mid[56:112], SIDE)
    side_c = over(mid[112:], SIDE)
    inward_last = cross(w_down[first_down:])
    inner_down = lax.ppermute(inward_down, EVERY, turned)
    inner_gate = lax.ppermute(inward_gate, EVERY, turned)
    far_a = over(side_a, MIRROR)
    inner_up = lax.ppermute(inward_up, EVERY, turned)
    home_own, mirror_own = own_hidden(mid), own_hidden(mirror)
    side_b, home_own, mirror_own = lax.optimization_barrier((side_b, home_own, mirror_own))
    far_b = over(side_b, MIRROR)
    far_c = over(side_c, MIRROR)
    inner_last = lax.ppermute(inward_last, EVERY, turned)

    outer = (place == 0) | (place == SPAN - 1)
    edge_gate = jnp.where(outer, outer_gate, inner_gate)
    edge_up = jnp.where(outer, outer_up, inner_up)
    edge_into = jnp.concatenate([edge_gate, edge_up], axis=1)
    side = jnp.concatenate([side_a, side_b, side_c], axis=0)
    far = jnp.concatenate(lax.optimization_barrier((far_a, far_b, far_c)), axis=0)

    def full_hidden(block, mine):
        both = dot(block, edge_into)
        edge_hidden = jax.nn.silu(both[:, :inner]) * both[:, inner:] * edge
        return jnp.concatenate([mine, edge_hidden.astype(jnp.bfloat16)], axis=1)

    pairs = ((far, own_hidden(far)), (mirror, mirror_own), (side, own_hidden(side)))
    tied = lax.optimization_barrier((outer_down, inner_down, inner_last, *[full_hidden(*p) for p in pairs]))
    edge_down = jnp.where(outer, tied[0], jnp.concatenate(tied[1:3], axis=0))
    down = jnp.concatenate([w_down, edge_down], axis=0)
    far = dot(tied[3], down).astype(jnp.bfloat16)
    far, mirror, side, mid, home_own = lax.optimization_barrier((far, *tied[4:], mid, home_own))
    mirror, side = [dot(h, down).astype(jnp.bfloat16) for h in (mirror, side)]
    home = dot(full_hidden(mid, home_own), down).astype(jnp.bfloat16)

    def added(u, v):
        return (u.astype(jnp.float32) + v.astype(jnp.float32)).astype(jnp.bfloat16)

    f32 = jnp.float32
    half = rows // 2
    upper, lower = slice(None, half), slice(half, None)
    result = None
    for lo, hi in ((0, 4096), (4096, width)):
        cols = slice(lo, hi)
        far_a = over(far[upper, cols], MIRROR)
        far_b = over(far[lower, cols], SIDE)
        mirror_a = over(mirror[upper, cols], MIRROR)
        side_b = over(side[lower, cols], SIDE)
        side_a = added(side[upper, cols], far_a)
        mirror_b = added(mirror[lower, cols], far_b)
        side_a = over(side_a, SIDE)
        mirror_b = over(mirror_b, MIRROR)
        total_a = home[upper, cols].astype(f32) + mirror_a.astype(f32) + side_a.astype(f32)
        total_b = home[lower, cols].astype(f32) + mirror_b.astype(f32) + side_b.astype(f32)
        total = jnp.concatenate([total_a, total_b], axis=0).astype(jnp.bfloat16)
        total = total.reshape(experts, CAPACITY, (hi - lo) // LANES, LANES)
        returned = lax.all_to_all(total, PLANE, 0, 0, tiled=True).reshape(rows, hi - lo)
        expert_out = lax.dot_general(picker, returned, (((0,), (0,)), ((), ())), preferred_element_type=f32)
        mixed = (expert_out * gate_prob.reshape(-1)[:, None]).astype(jnp.bfloat16)
        if result is None:
            result = lax.optimization_barrier(jnp.pad(mixed, ((0, 0), (0, width - hi))))
        else:
            result = lax.dynamic_update_slice(result, mixed, (0, lo))
    return result


def solution(mesh):
    grid = Mesh(mesh.devices.reshape(2, 4, 2, 2, 4), EVERY)
    spec2, spec3 = P(EVERY, None), P(EVERY, None, None)
    return jax.shard_map(
        body,
        mesh=grid,
        in_specs=(spec2, spec2, spec2, spec3, spec3, spec3, P()),
        out_specs=spec2,
        check_vma=False,
    )
```

```python
import jax
import jax.numpy as jnp
from jax import lax
from jax.sharding import Mesh, PartitionSpec as P


SPAN = 4
CAPACITY = 5
PLANE = ("zh", "y", "c", "zl")
EVERY = PLANE + ("x",)
LANES = 128
MIRROR = [(0, 3), (3, 0), (1, 2), (2, 1)]
SIDE = [(0, 1), (1, 0), (2, 3), (3, 2)]
INWARD = [(0, 1), (3, 2)]


def passing(last, first, experts):
    pairs = []
    for e in range(experts):
        pairs.append((SPAN * e + last, SPAN * ((e + 1) % experts) + last))
        pairs.append((SPAN * e + first, SPAN * ((e - 1) % experts) + first))
    return pairs


def multiplicities(partner, own, slots):
    expert, place = own // SPAN, own % SPAN
    start = expert * SPAN
    mine = lax.dynamic_slice_in_dim(partner, start, SPAN, 0)
    kept = jnp.sum((mine == own).astype(jnp.float32), axis=0)
    below = (mine[0] == (start - 1) % slots).astype(jnp.float32)
    above = (mine[SPAN - 1] == (start + SPAN) % slots).astype(jnp.float32)
    sent = jnp.stack([above[0], above[1], below[1], below[0]])
    return kept, sent[place]


def dot(a, b):
    return jnp.dot(a, b, preferred_element_type=jnp.float32)


def body(tokens, route, gate_prob, w_gate, w_up, w_down, partner):
    slots = lax.axis_size(EVERY)
    own = lax.axis_index(EVERY)
    experts = slots // SPAN
    place = lax.axis_index("x")
    width = tokens.shape[1]
    w_gate, w_up, w_down = w_gate[0], w_up[0], w_down[0]
    hidden = w_gate.shape[1]

    flat_route = route.reshape(-1)
    onehot = (flat_route[:, None] == jnp.arange(experts, dtype=jnp.int32)[None, :]).astype(jnp.int32)
    rank = jnp.sum(jnp.cumsum(onehot, axis=0) * onehot, axis=1) - 1
    row = flat_route * CAPACITY + rank
    rows = experts * CAPACITY
    picker = (jnp.arange(rows, dtype=jnp.int32)[:, None] == row[None, :]).astype(jnp.bfloat16)
    outgoing = dot(picker, tokens).astype(jnp.bfloat16)
    tiled = (experts, CAPACITY, width // LANES, LANES)
    outgoing = outgoing.reshape(tiled)
    inner = hidden // 2
    first_down = inner + 104
    straight, turned = passing(3, 0, experts), passing(2, 1, experts)

    def cross(block):
        return lax.ppermute(block, "x", INWARD)

    def over(block, pairs):
        return lax.ppermute(block, "x", pairs)

    inward_down = cross(w_down[inner:first_down])
    inward_gate = cross(w_gate[:, inner:])
    inward_up = cross(w_up[:, inner:])
    arrived = lax.all_to_all(outgoing, PLANE, 0, 0, tiled=True)
    mid = arrived.reshape(rows, width)

    kept, edge = multiplicities(partner, own, slots)
    scale = jnp.repeat(kept, inner)[None, :]

    def own_hidden(block):
        return (jax.nn.silu(dot(block, w_gate)) * dot(block, w_up) * scale).astype(jnp.bfloat16)

    mirror = over(mid, MIRROR)
    outer_gate = lax.ppermute(w_gate[:, :inner], EVERY, straight)
    outer_up = lax.ppermute(w_up[:, :inner], EVERY, straight)
    outer_down = lax.ppermute(w_down[:inner], EVERY, straight)
    side = []
    for name, lo in zip("abcd", range(0, rows, rows // 4)):
        side.append(over(mid[lo : lo + rows // 4], SIDE))
    inward_last = cross(w_down[first_down:])
    inner_down = lax.ppermute(inward_down, EVERY, turned)
    inner_gate = lax.ppermute(inward_gate, EVERY, turned)
    far = []
    far.append(over(side[0], MIRROR))
    inner_up = lax.ppermute(inward_up, EVERY, turned)
    home_own, mirror_own = own_hidden(mid), own_hidden(mirror)
    side[1], home_own, mirror_own = lax.optimization_barrier((side[1], home_own, mirror_own))
    for name, piece in zip("bcd", side[1:]):
        far.append(over(piece, MIRROR))
    inner_last = lax.ppermute(inward_last, EVERY, turned)

    outer = (place == 0) | (place == SPAN - 1)
    edge_gate = jnp.where(outer, outer_gate, inner_gate)
    edge_up = jnp.where(outer, outer_up, inner_up)
    edge_into = jnp.concatenate([edge_gate, edge_up], axis=1)
    side = jnp.concatenate(side, axis=0)
    far = jnp.concatenate(lax.optimization_barrier(tuple(far)), axis=0)

    def full_hidden(block, mine):
        both = dot(block, edge_into)
        edge_hidden = jax.nn.silu(both[:, :inner]) * both[:, inner:] * edge
        return jnp.concatenate([mine, edge_hidden.astype(jnp.bfloat16)], axis=1)

    pairs = ((far, own_hidden(far)), (mirror, mirror_own), (side, own_hidden(side)))
    tied = lax.optimization_barrier((outer_down, inner_down, inner_last, *[full_hidden(*p) for p in pairs]))
    edge_down = jnp.where(outer, tied[0], jnp.concatenate(tied[1:3], axis=0))
    down = jnp.concatenate([w_down, edge_down], axis=0)
    far = dot(tied[3], down).astype(jnp.bfloat16)
    far, mirror, side, mid, home_own = lax.optimization_barrier((far, *tied[4:], mid, home_own))
    mirror, side = [dot(h, down).astype(jnp.bfloat16) for h in (mirror, side)]
    home = dot(full_hidden(mid, home_own), down).astype(jnp.bfloat16)

    def added(u, v):
        return (u.astype(jnp.float32) + v.astype(jnp.float32)).astype(jnp.bfloat16)

    f32 = jnp.float32

    def placed(result, returned, lo):
        expert_out = lax.dot_general(picker, returned, (((0,), (0,)), ((), ())), preferred_element_type=f32)
        mixed = (expert_out * gate_prob.reshape(-1)[:, None]).astype(jnp.bfloat16)
        if result is None:
            return lax.optimization_barrier(jnp.pad(mixed, ((0, 0), (0, width - mixed.shape[1]))))
        return lax.dynamic_update_slice(result, mixed, (0, lo))

    result, returned = None, None
    for name, lo, hi in (("one", 0, 3072), ("two", 3072, 5120), ("three", 5120, width)):
        half = rows // 2 - (8 if name == "three" else 0)
        upper, lower, cols = slice(None, half), slice(half, None), slice(lo, hi)
        far_a = over(far[upper, cols], MIRROR)
        far_b = over(far[lower, cols], SIDE)
        mirror_a = over(mirror[upper, cols], MIRROR)
        side_b = over(side[lower, cols], SIDE)
        side_a = added(side[upper, cols], far_a)
        mirror_b = added(mirror[lower, cols], far_b)
        side_a = over(side_a, SIDE)
        mirror_b = over(mirror_b, MIRROR)
        total_a = home[upper, cols].astype(f32) + mirror_a.astype(f32) + side_a.astype(f32)
        total_b = home[lower, cols].astype(f32) + mirror_b.astype(f32) + side_b.astype(f32)
        total = jnp.concatenate([total_a, total_b], axis=0).astype(jnp.bfloat16)
        if returned is not None:
            total, returned = lax.optimization_barrier((total, returned))
            result = placed(result, returned, last)
        last = lo
        total = total.reshape(experts, CAPACITY, (hi - lo) // LANES, LANES)
        returned = lax.all_to_all(total, PLANE, 0, 0, tiled=True).reshape(rows, hi - lo)
    return placed(result, returned, last)


def solution(mesh):
    grid = Mesh(mesh.devices.reshape(2, 4, 2, 2, 4), EVERY)
    spec2, spec3 = P(EVERY, None), P(EVERY, None, None)
    return jax.shard_map(
        body,
        mesh=grid,
        in_specs=(spec2, spec2, spec2, spec3, spec3, spec3, P()),
        out_specs=spec2,
        check_vma=False,
    )
```
